256 devices in a mesh: gx: 8 (over y, core), gy: 8 (over z), gz: 4 (over x).
Axes of the slice: x: 4, y: 4, z: 8, core: 2. Of those that a mesh axis runs over, the one named last changes fastest.
Arguments:
- blocks: bfloat16 [1536, 64, 4096], P(('gx', 'gy', 'gz')), may hold values from -6 to 6
- ownership: int32 [1536, 3], P(('gx', 'gy', 'gz')), may hold values from -1 to 15, as said below
- basis_rows: bfloat16 [1024, 48], replicated, may hold values from -0.1875 to 0.1875
Outputs:
- gram_matrix: float32 [1024, 1024], P(('gx', 'gy', 'gz'))
The draws below stay inside these ranges and needn't reach their ends.
Inputs may be any that keep to these rules, and one draw needn't show every extreme that they name: `ownership`: row d * 6 + s is slot s of device d in mesh order. Each row is a block triple (i, j, k) with i <= j <= k, or -1 -1 -1 for an empty slot; every such triple of blocks 0 to 15 stands in exactly one row; the live slots of a device come first; some device has all 6 slots live.
All inputs are finite; a program needn't handle non-finite values.
Results may differ from the reference program's by a relative error of at most 0.0037.
Values may be sent and summed in bfloat16 or wider, within the bound.
No kernel may reach another device: no remote copies, remote signals or barrier semaphores. Data moves between devices by JAX's collectives and lax.ppermute only.
A program may use at most 128 MiB of HBM per device.

```python
import jax
import jax.numpy as jnp
import numpy as np
from jax import lax

N = 1024
NB = 16
R = 48
BS = 64
NUNIQ = 816
SLOTS = 6
DEVICES = 256


def draw_ownership(key, part):
    listing = np.array([[lead_block, mid_block, tail_block] for lead_block in range(NB) for mid_block in range(lead_block, NB) for tail_block in range(mid_block, NB)], dtype=np.int32)
    shuffled = jnp.asarray(listing)[jax.random.permutation(jax.random.fold_in(key, 11), listing.shape[0])]
    ranking = jax.random.permutation(jax.random.fold_in(key, 12), DEVICES)
    base_load = NUNIQ // DEVICES
    extra_load = NUNIQ % DEVICES
    loads = base_load + (ranking < extra_load).astype(jnp.int32) + jnp.where(ranking % 2 == 0, base_load - 1, 1 - base_load)
    offsets = jnp.cumsum(loads) - loads
    slot_ids = jnp.arange(SLOTS, dtype=jnp.int32)
    wanted = offsets[:, None] + slot_ids[None, :]
    live = slot_ids[None, :] < loads[:, None]
    selected_rows = shuffled[jnp.clip(wanted, 0, NUNIQ - 1)]
    return jnp.where(live[:, :, None], selected_rows, -1).reshape(DEVICES * SLOTS, 3).astype(jnp.int32)


def block_levels(stream_key, shape, pieces, smallest, largest):
    level = 1.0
    for dim, blocks in pieces:
        draws = jax.random.uniform(jax.random.fold_in(jax.random.fold_in(stream_key, 6), dim), (blocks,), jnp.float32, smallest / len(pieces), largest / len(pieces))
        level = level * jnp.repeat(jnp.exp(draws), shape[dim] // blocks).reshape((-1,) + (1,) * (len(shape) - 1 - dim))
    return level


def scatter_about(stream_key, dims, deviation, most, pieces=(), kind=jnp.bfloat16):
    values = deviation * jax.random.normal(stream_key, dims, jnp.float32)
    if pieces:
        values = values * block_levels(stream_key, dims, pieces, -0.22, 0.18)
    return jnp.clip(values, -most, most).astype(kind)


def setup_inputs(seed: int = 0) -> dict:
    arg_keys = jax.random.split(jax.random.key(seed), 4)
    blocks = scatter_about(arg_keys[0], (DEVICES * SLOTS, BS, BS * BS), 1.0, 6.0, ((0, 256),))
    ownership = draw_ownership(jax.random.fold_in(arg_keys[3], 71), 0)
    basis_rows = scatter_about(arg_keys[2], (N, R), N ** -0.5, 0.1875)
    return dict(blocks=blocks, ownership=ownership, basis_rows=basis_rows)


ORDERS = ((0, 1, 2), (0, 2, 1), (1, 0, 2), (1, 2, 0), (2, 0, 1), (2, 1, 0))
REDUCE_FORMS = ("gxyz,gxq->gyzq", "gxyz,gyq->gxzq", "gxyz,gzq->gxyq")


def unpack(stored, unique_triples):
    number = stored.shape[0]
    extent = stored.shape[1]
    unpacked = stored.reshape(number, extent, extent, extent)
    leading_block_index = lax.broadcasted_iota(jnp.int32, (1, extent, extent, extent), 1)
    middle = lax.broadcasted_iota(jnp.int32, (1, extent, extent, extent), 2)
    trailing = lax.broadcasted_iota(jnp.int32, (1, extent, extent, extent), 3)
    same_front = (unique_triples[:, 0] == unique_triples[:, 1])[:, None, None, None]
    same_back = (unique_triples[:, 1] == unique_triples[:, 2])[:, None, None, None]

    def order_back(values):
        return jnp.where(middle <= trailing, values, jnp.swapaxes(values, 2, 3))

    def order_front(values):
        return jnp.where(leading_block_index <= middle, values, jnp.swapaxes(values, 1, 2))

    unpacked = jnp.where(same_back, order_back(unpacked), unpacked)
    unpacked = jnp.where(same_front, order_front(unpacked), unpacked)
    unpacked = jnp.where(same_back, order_back(unpacked), unpacked)
    return unpacked


def slot_terms(stored, unique_triples, basis_rows):
    extent = stored.shape[1]
    columns = basis_rows.shape[1]
    unpacked = unpack(stored, unique_triples).astype(jnp.float32)
    basis_blocks = basis_rows.reshape(basis_rows.shape[0] // extent, extent, columns)
    selected_rows = jnp.take(basis_blocks, jnp.clip(unique_triples, 0, basis_blocks.shape[0] - 1), axis=0).astype(jnp.float32)
    factors = (selected_rows[:, 0], selected_rows[:, 1], selected_rows[:, 2])
    reduced = [jnp.einsum(REDUCE_FORMS[slot_pos], unpacked, factors[slot_pos]).astype(jnp.bfloat16).astype(jnp.float32) for slot_pos in range(3)]
    by_row = [0.0, 0.0, 0.0]
    for position in range(6):
        row_slot_index, middle_slot_index, last_slot = ORDERS[position]
        contraction_form = "zixl,zxo->ziol" if row_slot_index < middle_slot_index else "hwie,hwy->hiye"
        contrib = jnp.einsum(contraction_form, reduced[last_slot], factors[middle_slot_index])
        ordered = unique_triples[:, jnp.array(ORDERS[position])]
        distinct = unique_triples[:, 0] >= 0
        for earlier in ORDERS[:position]:
            distinct = distinct & jnp.any(ordered != unique_triples[:, jnp.array(earlier)], axis=1)
        by_row[row_slot_index] = by_row[row_slot_index] + jnp.where(distinct[:, None, None, None], contrib, 0.0)
    stacked = jnp.stack(by_row, axis=1)
    return stacked.reshape(stacked.shape[0], 3, extent, columns * columns)


def reference(blocks, ownership, basis_rows):
    extent = N // NB
    per_turn = 16
    turns = blocks.shape[0] // per_turn
    stored_all = blocks.reshape(turns, per_turn, extent, extent * extent)
    owned_all = ownership.reshape(turns, per_turn, 3)

    def scan_step(accumulated, scan_item):
        stored, unique_triples = scan_item
        contribs = slot_terms(stored, unique_triples, basis_rows)
        targets = jnp.clip(unique_triples, 0, NB - 1).reshape(-1).astype(jnp.int32)
        accumulated = accumulated.at[targets].add(contribs.reshape(-1, extent, R * R))
        return accumulated, None

    zero_rows = jnp.zeros((NB, extent, R * R), jnp.float32)
    summed, _ = lax.scan(scan_step, zero_rows, (stored_all, owned_all))
    product = summed.reshape(N, R, R)
    symmetric = (0.5 * (product + jnp.swapaxes(product, 1, 2))).reshape(N, R * R)
    rounded = symmetric.astype(jnp.bfloat16)
    return jnp.dot(rounded, rounded.T, preferred_element_type=jnp.float32) / R
```

```python
import jax
import jax.numpy as jnp
from jax import lax
from jax.experimental import pallas as pl
from jax.experimental.pallas import tpu as pltpu
from jax.sharding import Mesh
from jax.sharding import PartitionSpec as P

NB = 16
R = 48
BS = 64
HALF = BS // 2
PAIRS = R // 2
BLK = 8
QB = R // BLK
TRI = QB * (QB + 1) // 2
ROWS = TRI * BLK
LANES = 2 * BS
STRIDE = 104
F32 = jnp.float32
BF16 = jnp.bfloat16

NN = (((1,), (0,)), ((), ()))
NT = (((1,), (1,)), ((), ()))
TN = (((0,), (0,)), ((), ()))


def dot(a, b, dims=NN):
    return lax.dot_general(a, b, dims, preferred_element_type=F32)


def local_kernel(
    own, core, stored, basis, keep, send, acc, bases, masked, swapped, wide, with_y, with_x
):
    slot = pl.program_id(0)

    def low(rows):
        return lax.broadcasted_iota(jnp.int32, (rows, LANES), 1) < BS

    def tile(i):
        return slice(i * LANES, (i + 1) * LANES)

    def paired(first, second):
        mask = low(first.shape[0])
        return (
            jnp.where(mask, first, pltpu.roll(second, BS, 1)),
            jnp.where(mask, pltpu.roll(first, BS, 1), second),
        )

    def row_of_each(row):
        return wide[pl.ds(row, HALF, stride=STRIDE), :]

    @pl.when(slot == 0)
    def _():
        acc[...] = jnp.zeros_like(acc)
        for j in range(NB // 2):
            columns = basis[:, tile(j)]
            bases[2 * j] = columns[:, :BS]
            bases[2 * j + 1] = columns[:, BS:]

    v0 = own[slot, 0]
    v1 = own[slot, 1]
    v2 = own[slot, 2]

    @pl.when(v0 >= 0)
    def _():
        u0 = bases[v0]
        u1 = bases[v1]
        u2 = bases[v2]
        zero = jnp.zeros_like(u0)

        def twice(u):
            return jnp.concatenate(
                [jnp.concatenate([u, zero], 1), jnp.concatenate([zero, u], 1)], 0
            )

        both0 = twice(u0)
        both2 = twice(u2)
        both02 = jnp.concatenate([both0, both2], 1)

        for c in range(HALF // 2):
            first = stored[0, :, tile(c)].astype(F32)
            second = stored[0, :, tile(c + HALF // 2)].astype(F32)
            for k, part in enumerate(paired(first, second)):
                wide[(2 * c + k) * STRIDE : (2 * c + k) * STRIDE + BS, :] = part

        front = v0 == v1
        back = v1 == v2

        @pl.when(front | back)
        def _():
            x = lax.broadcasted_iota(jnp.int32, (BS, LANES), 0)
            lane = lax.broadcasted_iota(jnp.int32, (BS, LANES), 1)
            z = lane & (BS - 1)
            y_high = jnp.where(lane < BS, 0, HALF)

            def scale(i, carry):
                y = y_high + i
                dxy = jnp.where(front, x - y, -1)
                dyz = jnp.where(back, y - z, -1)
                w = jnp.where(dxy == 0, 0.5, 1.0) * jnp.where(dyz == 0, 0.5, 1.0)
                w = jnp.where((dxy == 0) & (dyz == 0), 1.0 / 6.0, w)
                w = jnp.where((dxy > 0) | (dyz > 0), 0.0, w)
                rows = pl.ds(pl.multiple_of(i * STRIDE, 8), BS)
                wide[rows, :] = wide[rows, :] * w
                return carry

            lax.fori_loop(0, HALF, scale, 0)

        for i in range(HALF):
            masked[:, tile(i)] = wide[i * STRIDE : i * STRIDE + BS, :].astype(BF16)
        for i in range(HALF):
            upper, lower = paired(row_of_each(i), row_of_each(i + HALF))
            swapped[:HALF, tile(i)] = upper.astype(BF16)
            swapped[HALF:, tile(i)] = lower.astype(BF16)

        def spread(values, target, place):
            for i in range(HALF):
                wide[i * STRIDE : i * STRIDE + R, :] = values[:, tile(i)]
            for j in range(PAIRS):
                upper, lower = paired(row_of_each(2 * j), row_of_each(2 * j + 1))
                target[:HALF, tile(place(j))] = upper.astype(BF16)
                target[HALF:, tile(place(j))] = lower.astype(BF16)

        spread(dot(u1, swapped[...]), with_x, lambda j: j)
        spread(dot(u0, masked[...]), with_y, lambda j: 2 * j + 1)
        for i in range(HALF):
            block = masked[:, tile(i)]
            wide[i * STRIDE : i * STRIDE + 2 * R, :] = dot(
                both2, jnp.concatenate([block, block], 0), NT
            )
        for j in range(PAIRS):
            for k in range(2):
                part = jnp.where(
                    low(HALF), row_of_each(k * R + 2 * j), row_of_each(k * R + 2 * j + 1)
                )
                with_y[k * HALF : (k + 1) * HALF, tile(2 * j)] = part.astype(BF16)

        def add(block, j, value):
            q = j // 4
            start = BLK * (q * (q + 1) // 2)
            rows = BLK * (q + 1)
            at = (block, j % 4, slice(start, start + rows), slice(None))
            acc[at] = acc[at] + value[:rows]

        for j in range(PAIRS):
            over_y = dot(u1, with_y[:, 2 * j * LANES : (2 * j + 2) * LANES])
            pair_x = with_x[:, tile(j)]
            pair_y = with_y[:, 2 * j * LANES : (2 * j + 2) * LANES]
            over_x = dot(u0, pair_x)
            lanes_x = dot(both2, jnp.concatenate([pair_x, pair_x], 0), NT)
            lanes_y = dot(both02, jnp.concatenate([pair_y, pair_y], 0), NT)
            keep_low = low(R)
            add(v0, j, over_y[:, :LANES] + jnp.where(keep_low, lanes_x[:R], lanes_x[R:]))
            add(v1, j, jnp.where(keep_low, lanes_y[:R], lanes_y[R:]))
            add(v2, j, over_y[:, LANES:] + over_x)

    @pl.when(slot == pl.num_programs(0) - 1)
    def _():
        mine = core[0]

        def write(m, carry):
            block = 4 * (m // 2) + m % 2
            keep[m // 2, :, m % 2] = acc[block + 2 * mine]
            send[m // 2, :, m % 2] = acc[block + 2 * (1 - mine)].astype(BF16)
            return carry

        lax.fori_loop(0, NB // 2, write, 0)


def local_products(blocks, ownership, basis, core):
    slots = blocks.shape[0]
    half = (4, 4, 2, ROWS, LANES)
    whole = pl.BlockSpec(half, lambda s, own, core: (0, 0, 0, 0, 0))
    return pl.pallas_call(
        local_kernel,
        grid_spec=pltpu.PrefetchScalarGridSpec(
            num_scalar_prefetch=2,
            grid=(slots,),
            in_specs=[
                pl.BlockSpec((1, BS, BS * BS), lambda s, own, core: (s, 0, 0)),
                pl.BlockSpec(basis.shape, lambda s, own, core: (0, 0)),
            ],
            out_specs=[whole, whole],
            scratch_shapes=[
                pltpu.VMEM((NB, 4, ROWS, LANES), F32),
                pltpu.VMEM((NB, R, BS), BF16),
                pltpu.VMEM((BS, BS * BS), BF16),
                pltpu.VMEM((BS, BS * BS), BF16),
                pltpu.VMEM((HALF * STRIDE, LANES), F32),
                pltpu.VMEM((BS, 2 * PAIRS * LANES), BF16),
                pltpu.VMEM((BS, PAIRS * LANES), BF16),
            ],
        ),
        out_shape=[jax.ShapeDtypeStruct(half, F32), jax.ShapeDtypeStruct(half, BF16)],
        compiler_params=pltpu.CompilerParams(vmem_limit_bytes=56 << 20),
        name="local_products",
    )(ownership, core, blocks, basis)


def local(blocks, ownership, basis_rows):
    core = lax.axis_index("gx_1").astype(jnp.int32).reshape(1)
    kept, sent = local_products(blocks, ownership, basis_rows.T, core)
    arrived = lax.ppermute(sent, "gx_1", [(0, 1), (1, 0)])
    pair = (kept + arrived.astype(F32)).astype(BF16)
    pieces = lax.all_to_all(
        pair.reshape(16, 2 * ROWS, LANES), ("gx_0", "gz"), 0, 0, tiled=True
    )
    plane = pieces.astype(F32).sum(axis=0)
    plane = plane.reshape(2 * TRI, BLK, LANES).swapaxes(0, 1)
    pieces = lax.all_to_all(plane, "gy", 0, 0, tiled=True)
    rounded = pieces.sum(axis=0).astype(BF16)
    rounded = rounded.reshape(2, TRI, 2, BS).transpose(2, 1, 0, 3).reshape(2 * TRI, LANES)
    tri = [2.0 if p < q else 1.0 for q in range(QB) for p in range(q + 1)]
    weight = jnp.array(tri + tri, BF16)[:, None]
    copies = jnp.broadcast_to(rounded, (8, 2 * TRI, LANES))
    gathered = lax.all_to_all(copies, ("gx_0", "gx_1"), 0, 0, tiled=True)
    gram = dot(rounded * weight, gathered, (((0,), (1,)), ((), ())))
    gram = gram.reshape(32, 4, 8 * LANES)
    pieces = lax.all_to_all(gram, ("gy", "gz"), 0, 0, tiled=True)
    return pieces.sum(axis=0) / R


def solution(mesh):
    split = Mesh(
        mesh.devices.reshape(4, 2, mesh.shape["gy"], mesh.shape["gz"]), ("gx_0", "gx_1", "gy", "gz")
    )
    axes = ("gx_0", "gx_1", "gy", "gz")
    return jax.shard_map(
        local,
        mesh=split,
        in_specs=(P(axes, None, None), P(axes, None), P()),
        out_specs=P(axes, None),
        check_vma=False,
    )
```

```python
import jax
import jax.numpy as jnp
from jax import lax
from jax.experimental import pallas as pl
from jax.experimental.pallas import tpu as pltpu
from jax.sharding import Mesh
from jax.sharding import PartitionSpec as P

NB = 16
R = 48
BS = 64
HALF = BS // 2
QUARTER = BS // 4
PAIRS = R // 2
BLK = 8
QB = R // BLK
TRI = QB * (QB + 1) // 2
ROWS = TRI * BLK
LANES = 2 * BS
STRIDE = 105
F32 = jnp.float32
BF16 = jnp.bfloat16

NN = (((1,), (0,)), ((), ()))
NT = (((1,), (1,)), ((), ()))
TN = (((0,), (0,)), ((), ()))


def dot(a, b, dims=NN):
    return lax.dot_general(a, b, dims, preferred_element_type=F32)


def local_kernel(
    own, core, stored, basis, keep, send, acc, bases, masked, swapped, wide, with_y, with_x
):
    slot = pl.program_id(0)

    def low(rows):
        return lax.broadcasted_iota(jnp.int32, (rows, LANES), 1) < BS

    def tile(i):
        return slice(i * LANES, (i + 1) * LANES)

    def paired(first, second):
        mask = low(first.shape[0])
        return (
            jnp.where(mask, first, pltpu.roll(second, BS, 1)),
            jnp.where(mask, pltpu.roll(first, BS, 1), second),
        )

    def row_of_each(row, count=HALF):
        return wide[pl.ds(row, count, stride=STRIDE), :]

    @pl.when(slot == 0)
    def _():
        acc[...] = jnp.zeros_like(acc)
        for j in range(NB // 2):
            columns = basis[:, tile(j)]
            bases[2 * j] = columns[:, :BS]
            bases[2 * j + 1] = columns[:, BS:]

    v0 = own[0, slot]
    v1 = own[1, slot]
    v2 = own[2, slot]

    @pl.when(v0 >= 0)
    def _():
        u0 = bases[v0]
        u1 = bases[v1]
        u2 = bases[v2]
        zero = jnp.zeros_like(u0)

        def twice(u):
            return jnp.concatenate(
                [jnp.concatenate([u, zero], 1), jnp.concatenate([zero, u], 1)], 0
            )

        both0 = twice(u0)
        both2 = twice(u2)
        both02 = jnp.concatenate([both0, both2], 1)

        for c in range(HALF // 2):
            first = stored[0, :, tile(c)].astype(F32)
            second = stored[0, :, tile(c + HALF // 2)].astype(F32)
            for k, part in enumerate(paired(first, second)):
                i = 2 * c + k
                wide[i * STRIDE : i * STRIDE + BS, :] = part
                masked[:, tile(i)] = part.astype(BF16)

        front = v0 == v1
        back = v1 == v2

        @pl.when(front | back)
        def _():
            x = lax.broadcasted_iota(jnp.int32, (BS, LANES), 0)
            lane = lax.broadcasted_iota(jnp.int32, (BS, LANES), 1)
            z = lane & (BS - 1)
            y_high = jnp.where(lane < BS, 0, HALF)

            def scale(i, carry):
                y = y_high + i
                dxy = jnp.where(front, x - y, -1)
                dyz = jnp.where(back, y - z, -1)
                w = jnp.where(dxy == 0, 0.5, 1.0) * jnp.where(dyz == 0, 0.5, 1.0)
                w = jnp.where((dxy == 0) & (dyz == 0), 1.0 / 6.0, w)
                w = jnp.where((dxy > 0) | (dyz > 0), 0.0, w)
                rows = pl.ds(i * STRIDE, BS)
                scaled = wide[rows, :] * w
                wide[rows, :] = scaled
                masked[:, pl.ds(pl.multiple_of(i * LANES, LANES), LANES)] = scaled.astype(BF16)
                return carry

            lax.fori_loop(0, HALF, scale, 0, unroll=4)

        for i in range(HALF):
            upper, lower = paired(row_of_each(i), row_of_each(i + HALF))
            swapped[:HALF, tile(i)] = upper.astype(BF16)
            swapped[HALF:, tile(i)] = lower.astype(BF16)

        def spread(values, target, place):
            for i in range(HALF):
                wide[i * STRIDE : i * STRIDE + R, :] = values[:, tile(i)]
            for j in range(PAIRS):
                upper, lower = paired(row_of_each(2 * j), row_of_each(2 * j + 1))
                target[:HALF, tile(place(j))] = upper.astype(BF16)
                target[HALF:, tile(place(j))] = lower.astype(BF16)

        spread(dot(u1, swapped[...]), with_x, lambda j: j)
        spread(dot(u0, masked[...]), with_y, lambda j: 2 * j + 1)
        for i in range(QUARTER):
            both_tiles = [masked[:, tile(i)], masked[:, tile(i + QUARTER)]]
            wide[i * STRIDE : i * STRIDE + 2 * R, :] = dot(
                both2, jnp.concatenate(both_tiles, 0), NT
            )
        for j in range(PAIRS):
            for k in range(2):
                parts = paired(
                    row_of_each(k * R + 2 * j, QUARTER), row_of_each(k * R + 2 * j + 1, QUARTER)
                )
                for h in range(2):
                    top = (2 * k + h) * QUARTER
                    with_y[top : top + QUARTER, tile(2 * j)] = parts[h].astype(BF16)

        def add(block, j, value):
            q = j // 4
            start = BLK * (q * (q + 1) // 2)
            rows = BLK * (q + 1)
            at = (block, j % 4, slice(start, start + rows), slice(None))
            acc[at] = acc[at] + value[:rows]

        def stacked(ref, tiles):
            return jnp.concatenate([ref[:, t] for t in tiles], 0)

        for g in range(QB // 2):
            rows = 2 * BLK * (g + 1)
            tiles = range(8 * g, 8 * g + 8)
            span_y = slice(16 * g * LANES, 16 * (g + 1) * LANES)
            span_x = slice(8 * g * LANES, 8 * (g + 1) * LANES)
            over_y = dot(u1[:rows], with_y[:, span_y])
            over_x = dot(u0[:rows], with_x[:, span_x])
            kept2 = jnp.concatenate([both2[:rows], both2[R : R + rows]], 0)
            kept02 = jnp.concatenate([both02[:rows], both02[R : R + rows]], 0)
            lanes_x = dot(kept2, stacked(with_x, [tile(j) for j in tiles]), NT)
            lanes_y = dot(
                kept02,
                stacked(with_y, [slice(2 * j * LANES, (2 * j + 2) * LANES) for j in tiles]),
                NT,
            )
            for k in range(4):
                from_x = paired(lanes_x[:rows, tile(k)], lanes_x[rows:, tile(k)])
                from_y = paired(lanes_y[:rows, tile(k)], lanes_y[rows:, tile(k)])
                for h in range(2):
                    i = 2 * k + h
                    j = 8 * g + i
                    add(v0, j, over_y[:, tile(2 * i)] + from_x[h])
                    add(v1, j, from_y[h])
                    add(v2, j, over_y[:, tile(2 * i + 1)] + over_x[:, tile(i)])

    @pl.when(slot == pl.num_programs(0) - 1)
    def _():
        mine = core[0]

        def write(m, carry):
            block = 4 * (m // 2) + m % 2
            keep[m // 2, :, m % 2] = acc[block + 2 * mine]
            send[m // 2, :, m % 2] = acc[block + 2 * (1 - mine)].astype(BF16)
            return carry

        lax.fori_loop(0, NB // 2, write, 0)


def local_products(blocks, ownership, basis, core):
    slots = blocks.shape[0]
    half = (4, 4, 2, ROWS, LANES)
    return pl.pallas_call(
        local_kernel,
        grid_spec=pltpu.PrefetchScalarGridSpec(
            num_scalar_prefetch=2,
            grid=(slots,),
            in_specs=[
                pl.BlockSpec((1, BS, BS * BS), lambda s, own, core: (s, 0, 0)),
                pl.BlockSpec(basis.shape, lambda s, own, core: (0, 0)),
            ],
            out_specs=[pl.BlockSpec(memory_space=pltpu.VMEM)] * 2,
            scratch_shapes=[
                pltpu.VMEM((NB, 4, ROWS, LANES), F32),
                pltpu.VMEM((NB, R, BS), BF16),
                pltpu.VMEM((BS, BS * BS), BF16),
                pltpu.VMEM((BS, BS * BS), BF16),
                pltpu.VMEM((HALF * STRIDE, LANES), F32),
                pltpu.VMEM((BS, 2 * PAIRS * LANES), BF16),
                pltpu.VMEM((BS, PAIRS * LANES), BF16),
            ],
        ),
        out_shape=[jax.ShapeDtypeStruct(half, F32), jax.ShapeDtypeStruct(half, BF16)],
        compiler_params=pltpu.CompilerParams(vmem_limit_bytes=48 << 20),
        name="local_products",
    )(ownership.T, core, blocks, basis)


def gram_kernel(mine, gathered, out):
    depth = mine.shape[0]
    low = lax.broadcasted_iota(jnp.int32, (depth, LANES), 1) < BS
    pair = lax.broadcasted_iota(jnp.int32, (depth, LANES), 0) // 2
    on_diagonal = pair < 0
    for q in range(QB):
        on_diagonal = on_diagonal | (pair == q * (q + 3) // 2)
    weighted = (mine[...].astype(F32) * jnp.where(on_diagonal, 1.0, 2.0)).astype(BF16)
    lows = []
    highs = []
    for g in range(0, NB, 2):
        first = gathered[g].astype(F32)
        second = gathered[g + 1].astype(F32)
        lows.append(jnp.where(low, first, pltpu.roll(second, BS, 1)).astype(BF16))
        highs.append(jnp.where(low, pltpu.roll(first, BS, 1), second).astype(BF16))
    gram = dot(weighted[:, :BS], jnp.concatenate(lows, 1), TN)
    gram = gram + dot(weighted[:, BS:], jnp.concatenate(highs, 1), TN)
    for i in range(16):
        out[i] = gram[4 * i : 4 * i + 4].astype(out.dtype)


def gram_part(mine, gathered):
    return pl.pallas_call(
        gram_kernel,
        in_specs=[pl.BlockSpec(memory_space=pltpu.VMEM)] * 2,
        out_specs=pl.BlockSpec(memory_space=pltpu.VMEM),
        out_shape=jax.ShapeDtypeStruct((16, 4, NB * BS), F32),
        compiler_params=pltpu.CompilerParams(vmem_limit_bytes=16 << 20),
        name="gram_part",
    )(mine, gathered)


def local(blocks, ownership, basis_rows):
    core = lax.axis_index("gx_1").astype(jnp.int32).reshape(1)
    kept, sent = local_products(blocks, ownership, basis_rows.T, core)
    arrived = lax.ppermute(sent, "gx_1", [(0, 1), (1, 0)])
    pair = (kept + arrived.astype(F32)).astype(BF16)
    pieces = lax.all_to_all(
        pair.reshape(16, 2 * ROWS, LANES), ("gx_0", "gz"), 0, 0, tiled=True
    )
    plane = pieces.astype(F32).sum(axis=0)
    plane = plane.reshape(2, TRI, 4, 2, LANES).transpose(0, 2, 1, 3, 4)
    plane = plane.reshape(8, 2 * TRI, LANES)
    pieces = lax.all_to_all(plane, ("gy_0", "gy_1"), 0, 0, tiled=True)
    rounded = pieces.sum(axis=0).astype(BF16)
    copies = jnp.broadcast_to(rounded, (16, 2 * TRI, LANES))
    gathered = lax.all_to_all(copies, ("gx_0", "gx_1", "gy_0"), 0, 0, tiled=True)
    pieces = lax.all_to_all(gram_part(rounded, gathered), ("gy_1", "gz"), 0, 0, tiled=True)
    return pieces.sum(axis=0) / R


def solution(mesh):
    axes = ("gx_0", "gx_1", "gy_0", "gy_1", "gz")
    split = Mesh(mesh.devices.reshape(4, 2, 2, 4, mesh.shape["gz"]), axes)
    return jax.shard_map(
        local,
        mesh=split,
        in_specs=(P(axes, None, None), P(axes, None), P()),
        out_specs=P(axes, None),
        check_vma=False,
    )
```

```python
import jax
import jax.numpy as jnp
from jax import lax
from jax.experimental import pallas as pl
from jax.experimental.pallas import tpu as pltpu
from jax.sharding import Mesh
from jax.sharding import PartitionSpec as P

NB = 16
R = 48
BS = 64
HALF = BS // 2
QUARTER = BS // 4
PAIRS = R // 2
BLK = 8
QB = R // BLK
TRI = QB * (QB + 1) // 2
ROWS = TRI * BLK
LANES = 2 * BS
STRIDE = 105
F32 = jnp.float32
BF16 = jnp.bfloat16

NN = (((1,), (0,)), ((), ()))
NT = (((1,), (1,)), ((), ()))
TN = (((0,), (0,)), ((), ()))


def dot(a, b, dims=NN):
    return lax.dot_general(a, b, dims, preferred_element_type=F32)


def local_kernel(
    own, core, stored, basis, keep, send, acc, bases, masked, swapped, wide, with_y, with_x
):
    slot = pl.program_id(0)

    def low(rows):
        return lax.broadcasted_iota(jnp.int32, (rows, LANES), 1) < BS

    def tile(i):
        return slice(i * LANES, (i + 1) * LANES)

    def paired(first, second):
        mask = low(first.shape[0])
        return (
            jnp.where(mask, first, pltpu.roll(second, BS, 1)),
            jnp.where(mask, pltpu.roll(first, BS, 1), second),
        )

    def row_of_each(row, count=HALF):
        return wide[pl.ds(row, count, stride=STRIDE), :]

    @pl.when(slot == 0)
    def _():
        acc[...] = jnp.zeros_like(acc)
        for j in range(NB // 2):
            columns = basis[:, tile(j)]
            bases[2 * j] = columns[:, :BS]
            bases[2 * j + 1] = columns[:, BS:]

    v0 = own[0, slot]
    v1 = own[1, slot]
    v2 = own[2, slot]

    @pl.when(v0 >= 0)
    def _():
        u0 = bases[v0]
        u1 = bases[v1]
        u2 = bases[v2]
        zero = jnp.zeros_like(u0)

        def twice(u):
            return jnp.concatenate(
                [jnp.concatenate([u, zero], 1), jnp.concatenate([zero, u], 1)], 0
            )

        both0 = twice(u0)
        both2 = twice(u2)
        both02 = jnp.concatenate([both0, both2], 1)

        for c in range(HALF // 2):
            first = stored[0, :, tile(c)].astype(F32)
            second = stored[0, :, tile(c + HALF // 2)].astype(F32)
            for k, part in enumerate(paired(first, second)):
                i = 2 * c + k
                wide[i * STRIDE : i * STRIDE + BS, :] = part
                masked[:, tile(i)] = part.astype(BF16)

        front = v0 == v1
        back = v1 == v2

        @pl.when(front | back)
        def _():
            x = lax.broadcasted_iota(jnp.int32, (BS, LANES), 0)
            lane = lax.broadcasted_iota(jnp.int32, (BS, LANES), 1)
            z = lane & (BS - 1)
            y_high = jnp.where(lane < BS, 0, HALF)

            def scale(i, carry):
                y = y_high + i
                dxy = jnp.where(front, x - y, -1)
                dyz = jnp.where(back, y - z, -1)
                w = jnp.where(dxy == 0, 0.5, 1.0) * jnp.where(dyz == 0, 0.5, 1.0)
                w = jnp.where((dxy == 0) & (dyz == 0), 1.0 / 6.0, w)
                w = jnp.where((dxy > 0) | (dyz > 0), 0.0, w)
                rows = pl.ds(i * STRIDE, BS)
                scaled = wide[rows, :] * w
                wide[rows, :] = scaled
                masked[:, pl.ds(pl.multiple_of(i * LANES, LANES), LANES)] = scaled.astype(BF16)
                return carry

            lax.fori_loop(0, HALF, scale, 0, unroll=4)

        for i in range(HALF):
            upper, lower = paired(row_of_each(i), row_of_each(i + HALF))
            swapped[:HALF, tile(i)] = upper.astype(BF16)
            swapped[HALF:, tile(i)] = lower.astype(BF16)

        def spread(values, target, place):
            for i in range(HALF):
                wide[i * STRIDE : i * STRIDE + R, :] = values[:, tile(i)]
            for j in range(PAIRS):
                upper, lower = paired(row_of_each(2 * j), row_of_each(2 * j + 1))
                target[:HALF, tile(place(j))] = upper.astype(BF16)
                target[HALF:, tile(place(j))] = lower.astype(BF16)

        spread(dot(u1, swapped[...]), with_x, lambda j: j)
        spread(dot(u0, masked[...]), with_y, lambda j: 2 * j + 1)
        for i in range(QUARTER):
            both_tiles = [masked[:, tile(i)], masked[:, tile(i + QUARTER)]]
            wide[i * STRIDE : i * STRIDE + 2 * R, :] = dot(
                both2, jnp.concatenate(both_tiles, 0), NT
            )
        for j in range(PAIRS):
            for k in range(2):
                parts = paired(
                    row_of_each(k * R + 2 * j, QUARTER), row_of_each(k * R + 2 * j + 1, QUARTER)
                )
                for h in range(2):
                    top = (2 * k + h) * QUARTER
                    with_y[top : top + QUARTER, tile(2 * j)] = parts[h].astype(BF16)

        def add(block, j, value):
            q = j // 4
            start = BLK * (q * (q + 1) // 2)
            rows = BLK * (q + 1)
            at = (block, j % 4, slice(start, start + rows), slice(None))
            acc[at] = acc[at] + value[:rows]

        def stacked(ref, tiles):
            return jnp.concatenate([ref[:, t] for t in tiles], 0)

        for g in range(QB // 2):
            rows = 2 * BLK * (g + 1)
            tiles = range(8 * g, 8 * g + 8)
            span_y = slice(16 * g * LANES, 16 * (g + 1) * LANES)
            span_x = slice(8 * g * LANES, 8 * (g + 1) * LANES)
            over_y = dot(u1[:rows], with_y[:, span_y])
            over_x = dot(u0[:rows], with_x[:, span_x])
            kept2 = jnp.concatenate([both2[:rows], both2[R : R + rows]], 0)
            kept02 = jnp.concatenate([both02[:rows], both02[R : R + rows]], 0)
            lanes_x = dot(kept2, stacked(with_x, [tile(j) for j in tiles]), NT)
            lanes_y = dot(
                kept02,
                stacked(with_y, [slice(2 * j * LANES, (2 * j + 2) * LANES) for j in tiles]),
                NT,
            )
            for k in range(4):
                from_x = paired(lanes_x[:rows, tile(k)], lanes_x[rows:, tile(k)])
                from_y = paired(lanes_y[:rows, tile(k)], lanes_y[rows:, tile(k)])
                for h in range(2):
                    i = 2 * k + h
                    j = 8 * g + i
                    add(v0, j, over_y[:, tile(2 * i)] + from_x[h])
                    add(v1, j, from_y[h])
                    add(v2, j, over_y[:, tile(2 * i + 1)] + over_x[:, tile(i)])

    @pl.when(slot == pl.num_programs(0) - 1)
    def _():
        mine = core[0]

        def write(m, carry):
            block = 4 * (m // 2) + m % 2
            keep[m // 2, :, m % 2] = acc[block + 2 * mine]
            send[m // 2, :, m % 2] = acc[block + 2 * (1 - mine)].astype(BF16)
            return carry

        lax.fori_loop(0, NB // 2, write, 0)


def in_hbm(array):
    return pltpu.with_memory_space_constraint(array, pltpu.HBM)


def local_products(blocks, ownership, basis, core):
    slots = blocks.shape[0]
    half = (4, 4, 2, ROWS, LANES)
    return pl.pallas_call(
        local_kernel,
        grid_spec=pltpu.PrefetchScalarGridSpec(
            num_scalar_prefetch=2,
            grid=(slots,),
            in_specs=[
                pl.BlockSpec((1, BS, BS * BS), lambda s, own, core: (s, 0, 0)),
                pl.BlockSpec(basis.shape, lambda s, own, core: (0, 0)),
            ],
            out_specs=[pl.BlockSpec(memory_space=pltpu.VMEM)] * 2,
            scratch_shapes=[
                pltpu.VMEM((NB, 4, ROWS, LANES), F32),
                pltpu.VMEM((NB, R, BS), BF16),
                pltpu.VMEM((BS, BS * BS), BF16),
                pltpu.VMEM((BS, BS * BS), BF16),
                pltpu.VMEM((HALF * STRIDE, LANES), F32),
                pltpu.VMEM((BS, 2 * PAIRS * LANES), BF16),
                pltpu.VMEM((BS, PAIRS * LANES), BF16),
            ],
        ),
        out_shape=[jax.ShapeDtypeStruct(half, F32), jax.ShapeDtypeStruct(half, BF16)],
        compiler_params=pltpu.CompilerParams(vmem_limit_bytes=48 << 20),
        name="local_products",
    )(in_hbm(ownership.T), core, blocks, in_hbm(basis))


def gram_kernel(mine, gathered, out):
    pair = lax.broadcasted_iota(jnp.int32, mine.shape, 0)
    pair = jnp.where(pair < TRI, pair, pair - TRI)
    on_diagonal = pair < 0
    for q in range(QB):
        on_diagonal = on_diagonal | (pair == q * (q + 3) // 2)
    weighted = (mine[...].astype(F32) * jnp.where(on_diagonal, 1.0, 2.0)).astype(BF16)
    everyone = jnp.concatenate([gathered[g] for g in range(gathered.shape[0])], 1)
    gram = dot(weighted, everyone, TN)
    for i in range(out.shape[0]):
        out[i] = gram[4 * i : 4 * i + 4].astype(out.dtype)


def gram_part(mine, gathered):
    return pl.pallas_call(
        gram_kernel,
        in_specs=[pl.BlockSpec(memory_space=pltpu.VMEM)] * 2,
        out_specs=pl.BlockSpec(memory_space=pltpu.VMEM),
        out_shape=jax.ShapeDtypeStruct((32, 4, NB * BS), BF16),
        compiler_params=pltpu.CompilerParams(vmem_limit_bytes=16 << 20),
        name="gram_part",
    )(mine, gathered)


def merge_kernel(pieces, out):
    total = pieces[0]
    for i in range(1, pieces.shape[0]):
        total = total + pieces[i]
    low = lax.broadcasted_iota(jnp.int32, (TRI, LANES), 1) < BS
    first = total[:TRI]
    second = total[TRI:]
    out[:TRI] = jnp.where(low, first, pltpu.roll(second, BS, 1)).astype(BF16)
    out[TRI:] = jnp.where(low, pltpu.roll(first, BS, 1), second).astype(BF16)


def merged(pieces):
    return pl.pallas_call(
        merge_kernel,
        in_specs=[pl.BlockSpec(memory_space=pltpu.VMEM)],
        out_specs=pl.BlockSpec(memory_space=pltpu.VMEM),
        out_shape=jax.ShapeDtypeStruct((2 * TRI, LANES), BF16),
        compiler_params=pltpu.CompilerParams(vmem_limit_bytes=16 << 20),
        name="merged",
    )(pieces)


def local(blocks, ownership, basis_rows):
    core = lax.axis_index("gx_1").astype(jnp.int32).reshape(1)
    kept, sent = local_products(blocks, ownership, basis_rows.T, core)
    arrived = lax.ppermute(sent, "gx_1", [(0, 1), (1, 0)])
    pair = (kept + arrived.astype(F32)).astype(BF16)
    pieces = lax.all_to_all(
        pair.reshape(16, 2 * ROWS, LANES), ("gx_0", "gz"), 0, 0, tiled=True
    )
    plane = pieces.astype(F32).sum(axis=0)
    plane = plane.reshape(2 * TRI, BLK, LANES).swapaxes(0, 1)
    pieces = lax.all_to_all(plane, "gy", 0, 0, tiled=True)
    rounded = merged(pieces)
    copies = jnp.broadcast_to(rounded, (8, 2 * TRI, LANES))
    gathered = lax.all_to_all(copies, ("gx_0", "gx_1"), 0, 0, tiled=True)
    pieces = lax.all_to_all(gram_part(rounded, gathered), ("gy", "gz"), 0, 0, tiled=True)
    return pieces.astype(F32).sum(axis=0) / R


def solution(mesh):
    axes = ("gx_0", "gx_1", "gy", "gz")
    split = Mesh(mesh.devices.reshape(4, 2, mesh.shape["gy"], mesh.shape["gz"]), axes)
    return jax.shard_map(
        local,
        mesh=split,
        in_specs=(P(axes, None, None), P(axes, None), P()),
        out_specs=P(axes, None),
        check_vma=False,
    )
```

```python
import jax
import jax.numpy as jnp
from jax import lax
from jax.experimental import pallas as pl
from jax.experimental.pallas import tpu as pltpu
from jax.sharding import Mesh
from jax.sharding import PartitionSpec as P

NB = 16
R = 48
BS = 64
HALF = BS // 2
QUARTER = BS // 4
PAIRS = R // 2
BLK = 8
QB = R // BLK
TRI = QB * (QB + 1) // 2
ROWS = TRI * BLK
LANES = 2 * BS
STRIDE = 105
F32 = jnp.float32
BF16 = jnp.bfloat16

ORDER_Y = (2, 3, 0, 1)
ORDER_X = (2, 0, 3, 1)
ORDER_Z = (4, 5, 6, 7, 0, 1, 2, 3)
ORDER_YC = (4, 5, 6, 7, 0, 1, 2, 3)
ORDER_ZX = tuple(4 * z + x for z in ORDER_Z for x in ORDER_X)

NN = (((1,), (0,)), ((), ()))
NT = (((1,), (1,)), ((), ()))
TN = (((0,), (0,)), ((), ()))


def dot(a, b, dims=NN):
    return lax.dot_general(a, b, dims, preferred_element_type=F32)


def local_kernel(
    own, core, stored, basis, acc, send, bases, masked, swapped, wide, wide1, wide0, wide2, with_y, with_x
):
    slot = pl.program_id(0)

    def low(rows):
        return lax.broadcasted_iota(jnp.int32, (rows, LANES), 1) < BS

    def tile(i):
        return slice(i * LANES, (i + 1) * LANES)

    def paired(first, second):
        mask = low(first.shape[0])
        return (
            jnp.where(mask, first, pltpu.roll(second, BS, 1)),
            jnp.where(mask, pltpu.roll(first, BS, 1), second),
        )

    def row_of_each(ref, row, count=HALF):
        return ref[pl.ds(row, count, stride=STRIDE), :]

    @pl.when(slot == 0)
    def _():
        acc[...] = jnp.zeros_like(acc)
        for j in range(NB // 2):
            columns = basis[:, tile(j)]
            bases[2 * j] = columns[:, :BS]
            bases[2 * j + 1] = columns[:, BS:]

    v0 = own[0, slot]
    v1 = own[1, slot]
    v2 = own[2, slot]

    @pl.when(v0 >= 0)
    def _():
        u0 = bases[v0]
        u1 = bases[v1]
        u2 = bases[v2]
        zero = jnp.zeros_like(u0)

        def twice(u):
            return jnp.concatenate(
                [jnp.concatenate([u, zero], 1), jnp.concatenate([zero, u], 1)], 0
            )

        both0 = twice(u0)
        both2 = twice(u2)
        both02 = jnp.concatenate([both0, both2], 1)

        for c in range(HALF // 2):
            first = stored[0, :, tile(c)].astype(F32)
            second = stored[0, :, tile(c + HALF // 2)].astype(F32)
            for k, part in enumerate(paired(first, second)):
                i = 2 * c + k
                wide[i * STRIDE : i * STRIDE + BS, :] = part
                masked[:, tile(i)] = part.astype(BF16)

        front = v0 == v1
        back = v1 == v2

        @pl.when(front | back)
        def _():
            x = lax.broadcasted_iota(jnp.int32, (BS, LANES), 0)
            lane = lax.broadcasted_iota(jnp.int32, (BS, LANES), 1)
            z = lane & (BS - 1)
            y_high = jnp.where(lane < BS, 0, HALF)
            order_xy = jnp.where(front, (y_high - x).astype(F32) * 0.5 + 0.5, 2.0 * BS)
            order_yz = jnp.where(back, (z - y_high).astype(F32) * 0.5 + 0.5, 2.0 * BS)

            def scale(i, carry):
                step = i.astype(F32) * 0.5
                w = jnp.clip(order_xy + step, 0.0, 1.0) * jnp.clip(order_yz - step, 0.0, 1.0)
                w = jnp.where(w == 0.25, 1.0 / 6.0, w)
                rows = pl.ds(i * STRIDE, BS)
                scaled = wide[rows, :] * w
                wide[rows, :] = scaled
                masked[:, pl.ds(pl.multiple_of(i * LANES, LANES), LANES)] = scaled.astype(BF16)
                return carry

            lax.fori_loop(0, HALF, scale, 0, unroll=4)

        for i in range(HALF):
            upper, lower = paired(row_of_each(wide, i), row_of_each(wide, i + HALF))
            swapped[:HALF, tile(i)] = upper.astype(BF16)
            swapped[HALF:, tile(i)] = lower.astype(BF16)

        def spread(values, ref, target, place):
            for i in range(HALF):
                ref[i * STRIDE : i * STRIDE + R, :] = values[:, tile(i)]
            for j in range(PAIRS):
                upper, lower = paired(row_of_each(ref, 2 * j), row_of_each(ref, 2 * j + 1))
                target[:HALF, tile(place(j))] = upper.astype(BF16)
                target[HALF:, tile(place(j))] = lower.astype(BF16)

        spread(dot(u1, swapped[...]), wide1, with_x, lambda j: j)
        spread(dot(u0, masked[...]), wide0, with_y, lambda j: 2 * j + 1)
        for i in range(QUARTER):
            both_tiles = [masked[:, tile(i)], masked[:, tile(i + QUARTER)]]
            wide2[i * STRIDE : i * STRIDE + 2 * R, :] = dot(
                both2, jnp.concatenate(both_tiles, 0), NT
            )
        for j in range(PAIRS):
            for k in range(2):
                parts = paired(
                    row_of_each(wide2, k * R + 2 * j, QUARTER),
                    row_of_each(wide2, k * R + 2 * j + 1, QUARTER),
                )
                for h in range(2):
                    top = (2 * k + h) * QUARTER
                    with_y[top : top + QUARTER, tile(2 * j)] = parts[h].astype(BF16)

        def place(v):
            group = sum(jnp.where(v // 4 == y, i, 0) for i, y in enumerate(ORDER_Y))
            return ((v // 2) % 2) ^ core[0], group, v % 2

        places = [place(v) for v in (v0, v1, v2)]

        def add(f, j, value):
            side, group, half = places[f]
            block = (side, group, j % 4, half)
            q = j // 4
            start = BLK * (q * (q + 1) // 2)
            rows = BLK * (q + 1)
            at = (*block, slice(start, start + rows), slice(None))
            acc[at] = acc[at] + value[:rows]

        def stacked(ref, tiles):
            return jnp.concatenate([ref[:, t] for t in tiles], 0)

        for g in range(QB // 2):
            rows = 2 * BLK * (g + 1)
            tiles = range(8 * g, 8 * g + 8)
            span_y = slice(16 * g * LANES, 16 * (g + 1) * LANES)
            span_x = slice(8 * g * LANES, 8 * (g + 1) * LANES)
            over_y = dot(u1[:rows], with_y[:, span_y])
            over_x = dot(u0[:rows], with_x[:, span_x])
            kept2 = jnp.concatenate([both2[:rows], both2[R : R + rows]], 0)
            kept02 = jnp.concatenate([both02[:rows], both02[R : R + rows]], 0)
            lanes_x = dot(kept2, stacked(with_x, [tile(j) for j in tiles]), NT)
            lanes_y = dot(
                kept02,
                stacked(with_y, [slice(2 * j * LANES, (2 * j + 2) * LANES) for j in tiles]),
                NT,
            )
            for k in range(4):
                from_x = paired(lanes_x[:rows, tile(k)], lanes_x[rows:, tile(k)])
                from_y = paired(lanes_y[:rows, tile(k)], lanes_y[rows:, tile(k)])
                for h in range(2):
                    i = 2 * k + h
                    j = 8 * g + i
                    add(0, j, over_y[:, tile(2 * i)] + from_x[h])
                    add(1, j, from_y[h])
                    add(2, j, over_y[:, tile(2 * i + 1)] + over_x[:, tile(i)])

    @pl.when(slot == pl.num_programs(0) - 1)
    def _():
        def write(m, carry):
            send[m] = acc[1, m].astype(BF16)
            return carry

        lax.fori_loop(0, 4, write, 0)


def in_hbm(array):
    return pltpu.with_memory_space_constraint(array, pltpu.HBM)


def local_products(blocks, ownership, basis, core):
    slots = blocks.shape[0]
    half = (4, 4, 2, ROWS, LANES)
    return pl.pallas_call(
        local_kernel,
        grid_spec=pltpu.PrefetchScalarGridSpec(
            num_scalar_prefetch=2,
            grid=(slots,),
            in_specs=[
                pl.BlockSpec((1, BS, BS * BS), lambda s, own, core: (s, 0, 0)),
                pl.BlockSpec(basis.shape, lambda s, own, core: (0, 0)),
            ],
            out_specs=[pl.BlockSpec(memory_space=pltpu.VMEM)] * 2,
            scratch_shapes=[
                pltpu.VMEM((NB, R, BS), BF16),
                pltpu.VMEM((BS, BS * BS), BF16),
                pltpu.VMEM((BS, BS * BS), BF16),
                pltpu.VMEM((HALF * STRIDE, LANES), F32),
                pltpu.VMEM((HALF * STRIDE, LANES), F32),
                pltpu.VMEM((HALF * STRIDE, LANES), F32),
                pltpu.VMEM((QUARTER * STRIDE, LANES), F32),
                pltpu.VMEM((BS, 2 * PAIRS * LANES), BF16),
                pltpu.VMEM((BS, PAIRS * LANES), BF16),
            ],
        ),
        out_shape=[
            jax.ShapeDtypeStruct((2, *half), F32),
            jax.ShapeDtypeStruct(half, BF16),
        ],
        compiler_params=pltpu.CompilerParams(vmem_limit_bytes=36 << 20),
        name="local_products",
    )(in_hbm(ownership.T), core, in_hbm(blocks), in_hbm(basis))


def gram_kernel(mine, gathered, out):
    pair = lax.broadcasted_iota(jnp.int32, mine.shape, 0)
    pair = jnp.where(pair < TRI, pair, pair - TRI)
    on_diagonal = pair < 0
    for q in range(QB):
        on_diagonal = on_diagonal | (pair == q * (q + 3) // 2)
    weighted = (mine[...].astype(F32) * jnp.where(on_diagonal, 1.0, 2.0)).astype(BF16)
    everyone = jnp.concatenate([gathered[ORDER_YC.index(g)] for g in range(len(ORDER_YC))], 1)
    gram = dot(weighted, everyone, TN) / R
    for i, place in enumerate(ORDER_ZX):
        out[i] = gram[4 * place : 4 * place + 4].astype(out.dtype)


def gram_part(mine, gathered):
    return pl.pallas_call(
        gram_kernel,
        in_specs=[pl.BlockSpec(memory_space=pltpu.VMEM)] * 2,
        out_specs=pl.BlockSpec(memory_space=pltpu.VMEM),
        out_shape=jax.ShapeDtypeStruct((32, 4, NB * BS), BF16),
        compiler_params=pltpu.CompilerParams(vmem_limit_bytes=16 << 20),
        name="gram_part",
    )(mine, gathered)


def merge_kernel(pieces, out, copies):
    total = pieces[0]
    for i in range(1, pieces.shape[0]):
        total = total + pieces[i]
    low = lax.broadcasted_iota(jnp.int32, (TRI, LANES), 1) < BS
    first = total[:TRI]
    second = total[TRI:]
    upper = jnp.where(low, first, pltpu.roll(second, BS, 1)).astype(BF16)
    lower = jnp.where(low, pltpu.roll(first, BS, 1), second).astype(BF16)
    for ref in (out, *(copies.at[g] for g in range(copies.shape[0]))):
        ref[:TRI] = upper
        ref[TRI:] = lower


def merged(pieces):
    return pl.pallas_call(
        merge_kernel,
        in_specs=[pl.BlockSpec(memory_space=pltpu.VMEM)],
        out_specs=[pl.BlockSpec(memory_space=pltpu.VMEM)] * 2,
        out_shape=[
            jax.ShapeDtypeStruct((2 * TRI, LANES), BF16),
            jax.ShapeDtypeStruct((8, 2 * TRI, LANES), BF16),
        ],
        compiler_params=pltpu.CompilerParams(vmem_limit_bytes=16 << 20),
        name="merged",
    )(pieces)


def exchange(pieces, axes, order):
    return lax.all_to_all(
        pieces, axes, 0, 0, axis_index_groups=[list(order)], tiled=True
    )


def local(blocks, ownership, basis_rows):
    core = lax.axis_index("gx_1").astype(jnp.int32).reshape(1)
    kept, sent = local_products(blocks, ownership, basis_rows.T, core)
    arrived = lax.ppermute(sent, "gx_1", [(0, 1), (1, 0)])
    pair = (kept[0] + arrived.astype(F32)).astype(BF16)
    ranks = [4 * y + x for y in ORDER_Y for x in ORDER_X]
    pieces = exchange(pair.reshape(16, 2 * ROWS, LANES), ("gx_0", "gz"), ranks)
    plane = pieces.astype(F32).sum(axis=0)
    plane = plane.reshape(2 * TRI, BLK, LANES).swapaxes(0, 1)
    rounded, copies = merged(exchange(plane, "gy", ORDER_Z))
    gathered = exchange(copies, ("gx_0", "gx_1"), ORDER_YC)
    pieces = exchange(gram_part(rounded, gathered), ("gy", "gz"), ORDER_ZX)
    return pieces.astype(F32).sum(axis=0)


def solution(mesh):
    axes = ("gx_0", "gx_1", "gy", "gz")
    split = Mesh(mesh.devices.reshape(4, 2, mesh.shape["gy"], mesh.shape["gz"]), axes)
    return jax.shard_map(
        local,
        mesh=split,
        in_specs=(P(axes, None, None), P(axes, None), P()),
        out_specs=P(axes, None),
        check_vma=False,
    )
```

```python
import jax
import jax.numpy as jnp
from jax import lax
from jax.experimental import pallas as pl
from jax.experimental.pallas import tpu as pltpu
from jax.sharding import Mesh
from jax.sharding import PartitionSpec as P

NB = 16
R = 48
BS = 64
HALF = BS // 2
QUARTER = BS // 4
PAIRS = R // 2
BLK = 8
QB = R // BLK
TRI = QB * (QB + 1) // 2
ROWS = TRI * BLK
LANES = 2 * BS
STRIDE = 105
F32 = jnp.float32
BF16 = jnp.bfloat16

ORDER_Y = (2, 3, 0, 1)
ORDER_X = (2, 0, 3, 1)
ORDER_Z = (4, 5, 6, 7, 2, 3, 0, 1)
ORDER_YC = (4, 5, 6, 7, 2, 3, 0, 1)
ORDER_ZX = tuple(4 * z + x for z in (4, 5, 6, 7, 0, 1, 2, 3) for x in ORDER_X)

NN = (((1,), (0,)), ((), ()))
NT = (((1,), (1,)), ((), ()))
TN = (((0,), (0,)), ((), ()))


def dot(a, b, dims=NN):
    return lax.dot_general(a, b, dims, preferred_element_type=F32)


def local_kernel(
    own, core, blocks, basis_hbm, acc, send,
    stored, basis, arrived, bases, masked, swapped, wide, wide1, wide0, wide2, with_y, with_x,
):
    slots = blocks.shape[0]

    def low(rows):
        return lax.broadcasted_iota(jnp.int32, (rows, LANES), 1) < BS

    def tile(i):
        return slice(i * LANES, (i + 1) * LANES)

    def paired(first, second):
        mask = low(first.shape[0])
        return (
            jnp.where(mask, first, pltpu.roll(second, BS, 1)),
            jnp.where(mask, pltpu.roll(first, BS, 1), second),
        )

    def row_of_each(ref, row, count=HALF):
        return ref[pl.ds(row, count, stride=STRIDE), :]

    def fetch(slot):
        return pltpu.make_async_copy(blocks.at[slot], stored.at[slot], arrived.at[slot])

    fetch_basis = pltpu.make_async_copy(basis_hbm, basis, arrived.at[slots])
    fetch_basis.start()
    for slot in range(slots):
        fetch(slot).start()
    acc[...] = jnp.zeros_like(acc)
    fetch_basis.wait()
    for j in range(NB // 2):
        columns = basis[:, tile(j)]
        bases[2 * j] = columns[:, :BS]
        bases[2 * j + 1] = columns[:, BS:]

    def each_slot(slot, carry):
        fetch(slot).wait()
        one_slot(slot)
        return carry

    def one_slot(slot):
        v0 = own[0, slot]
        v1 = own[1, slot]
        v2 = own[2, slot]

        @pl.when(v0 >= 0)
        def _():
            u0 = bases[v0]
            u1 = bases[v1]
            u2 = bases[v2]
            zero = jnp.zeros_like(u0)

            def twice(u):
                return jnp.concatenate(
                    [jnp.concatenate([u, zero], 1), jnp.concatenate([zero, u], 1)], 0
                )

            both0 = twice(u0)
            both2 = twice(u2)
            both02 = jnp.concatenate([both0, both2], 1)

            for c in range(HALF // 2):
                first = stored[slot, :, tile(c)].astype(F32)
                second = stored[slot, :, tile(c + HALF // 2)].astype(F32)
                for k, part in enumerate(paired(first, second)):
                    i = 2 * c + k
                    wide[i * STRIDE : i * STRIDE + BS, :] = part
                    masked[:, tile(i)] = part.astype(BF16)

            front = v0 == v1
            back = v1 == v2

            @pl.when(front | back)
            def _():
                x = lax.broadcasted_iota(jnp.int32, (BS, LANES), 0)
                lane = lax.broadcasted_iota(jnp.int32, (BS, LANES), 1)
                z = lane & (BS - 1)
                y_high = jnp.where(lane < BS, 0, HALF)
                order_xy = jnp.where(front, (y_high - x).astype(F32) * 0.5 + 0.5, 2.0 * BS)
                order_yz = jnp.where(back, (z - y_high).astype(F32) * 0.5 + 0.5, 2.0 * BS)

                def scale(i, carry):
                    step = i.astype(F32) * 0.5
                    w = jnp.clip(order_xy + step, 0.0, 1.0) * jnp.clip(order_yz - step, 0.0, 1.0)
                    w = jnp.where(w == 0.25, 1.0 / 6.0, w)
                    rows = pl.ds(i * STRIDE, BS)
                    scaled = wide[rows, :] * w
                    wide[rows, :] = scaled
                    masked[:, pl.ds(pl.multiple_of(i * LANES, LANES), LANES)] = scaled.astype(BF16)
                    return carry

                lax.fori_loop(0, HALF, scale, 0, unroll=4)

            for i in range(HALF):
                upper, lower = paired(row_of_each(wide, i), row_of_each(wide, i + HALF))
                swapped[:HALF, tile(i)] = upper.astype(BF16)
                swapped[HALF:, tile(i)] = lower.astype(BF16)

            def spread(values, ref, target, place):
                for i in range(HALF):
                    ref[i * STRIDE : i * STRIDE + R, :] = values[:, tile(i)]
                for j in range(PAIRS):
                    upper, lower = paired(row_of_each(ref, 2 * j), row_of_each(ref, 2 * j + 1))
                    target[:HALF, tile(place(j))] = upper.astype(BF16)
                    target[HALF:, tile(place(j))] = lower.astype(BF16)

            spread(dot(u1, swapped[...]), wide1, with_x, lambda j: j)
            spread(dot(u0, masked[...]), wide0, with_y, lambda j: 2 * j + 1)
            for i in range(QUARTER):
                both_tiles = [masked[:, tile(i)], masked[:, tile(i + QUARTER)]]
                wide2[i * STRIDE : i * STRIDE + 2 * R, :] = dot(
                    both2, jnp.concatenate(both_tiles, 0), NT
                )
            for j in range(PAIRS):
                for k in range(2):
                    parts = paired(
                        row_of_each(wide2, k * R + 2 * j, QUARTER),
                        row_of_each(wide2, k * R + 2 * j + 1, QUARTER),
                    )
                    for h in range(2):
                        top = (2 * k + h) * QUARTER
                        with_y[top : top + QUARTER, tile(2 * j)] = parts[h].astype(BF16)

            def place(v):
                group = sum(jnp.where(v // 4 == y, i, 0) for i, y in enumerate(ORDER_Y))
                return ((v // 2) % 2) ^ core[0], group, v % 2

            places = [place(v) for v in (v0, v1, v2)]

            def add(f, j, value):
                side, group, half = places[f]
                block = (side, group, j % 4, half)
                q = j // 4
                start = BLK * (q * (q + 1) // 2)
                rows = BLK * (q + 1)
                at = (*block, slice(start, start + rows), slice(None))
                acc[at] = acc[at] + value[:rows]

            def stacked(ref, tiles):
                return jnp.concatenate([ref[:, t] for t in tiles], 0)

            for g in range(QB // 2):
                rows = 2 * BLK * (g + 1)
                tiles = range(8 * g, 8 * g + 8)
                span_y = slice(16 * g * LANES, 16 * (g + 1) * LANES)
                span_x = slice(8 * g * LANES, 8 * (g + 1) * LANES)
                over_y = dot(u1[:rows], with_y[:, span_y])
                over_x = dot(u0[:rows], with_x[:, span_x])
                kept2 = jnp.concatenate([both2[:rows], both2[R : R + rows]], 0)
                kept02 = jnp.concatenate([both02[:rows], both02[R : R + rows]], 0)
                lanes_x = dot(kept2, stacked(with_x, [tile(j) for j in tiles]), NT)
                lanes_y = dot(
                    kept02,
                    stacked(with_y, [slice(2 * j * LANES, (2 * j + 2) * LANES) for j in tiles]),
                    NT,
                )
                for k in range(4):
                    from_x = paired(lanes_x[:rows, tile(k)], lanes_x[rows:, tile(k)])
                    from_y = paired(lanes_y[:rows, tile(k)], lanes_y[rows:, tile(k)])
                    for h in range(2):
                        i = 2 * k + h
                        j = 8 * g + i
                        add(0, j, over_y[:, tile(2 * i)] + from_x[h])
                        add(1, j, from_y[h])
                        add(2, j, over_y[:, tile(2 * i + 1)] + over_x[:, tile(i)])

    lax.fori_loop(0, slots, each_slot, 0)

    def write(m, carry):
        send[m] = acc[1, m].astype(BF16)
        return carry

    lax.fori_loop(0, 4, write, 0)


def in_hbm(array):
    return pltpu.with_memory_space_constraint(array, pltpu.HBM)


def local_products(blocks, ownership, basis, core):
    slots = blocks.shape[0]
    half = (4, 4, 2, ROWS, LANES)
    in_vmem = pl.BlockSpec(memory_space=pltpu.VMEM)
    in_smem = pl.BlockSpec(memory_space=pltpu.SMEM)
    outside = pl.BlockSpec(memory_space=pltpu.HBM)
    return pl.pallas_call(
        local_kernel,
        in_specs=[in_smem, in_smem, outside, outside],
        out_specs=[in_vmem, in_vmem],
        scratch_shapes=[
            pltpu.VMEM(blocks.shape, BF16),
            pltpu.VMEM(basis.shape, BF16),
            pltpu.SemaphoreType.DMA((slots + 1,)),
            pltpu.VMEM((NB, R, BS), BF16),
            pltpu.VMEM((BS, BS * BS), BF16),
            pltpu.VMEM((BS, BS * BS), BF16),
            pltpu.VMEM((HALF * STRIDE, LANES), F32),
            pltpu.VMEM((HALF * STRIDE, LANES), F32),
            pltpu.VMEM((HALF * STRIDE, LANES), F32),
            pltpu.VMEM((QUARTER * STRIDE, LANES), F32),
            pltpu.VMEM((BS, 2 * PAIRS * LANES), BF16),
            pltpu.VMEM((BS, PAIRS * LANES), BF16),
        ],
        out_shape=[
            jax.ShapeDtypeStruct((2, *half), F32),
            jax.ShapeDtypeStruct(half, BF16),
        ],
        compiler_params=pltpu.CompilerParams(vmem_limit_bytes=36 << 20),
        name="local_products",
    )(in_hbm(ownership.T), core, in_hbm(blocks), in_hbm(basis))


def gram_kernel(mine, gathered, out):
    pair = lax.broadcasted_iota(jnp.int32, mine.shape, 0)
    pair = jnp.where(pair < TRI, pair, pair - TRI)
    on_diagonal = pair < 0
    for q in range(QB):
        on_diagonal = on_diagonal | (pair == q * (q + 3) // 2)
    weighted = (mine[...].astype(F32) * jnp.where(on_diagonal, 1.0, 2.0)).astype(BF16)
    everyone = jnp.concatenate([gathered[ORDER_YC.index(g)] for g in range(len(ORDER_YC))], 1)
    gram = dot(weighted, everyone, TN) / R
    for i, place in enumerate(ORDER_ZX):
        out[i] = gram[4 * place : 4 * place + 4].astype(out.dtype)


def gram_part(mine, gathered):
    return pl.pallas_call(
        gram_kernel,
        in_specs=[pl.BlockSpec(memory_space=pltpu.VMEM)] * 2,
        out_specs=pl.BlockSpec(memory_space=pltpu.VMEM),
        out_shape=jax.ShapeDtypeStruct((32, 4, NB * BS), BF16),
        compiler_params=pltpu.CompilerParams(vmem_limit_bytes=16 << 20),
        name="gram_part",
    )(mine, gathered)


def merge_kernel(pieces, out, copies):
    total = pieces[0]
    for i in range(1, pieces.shape[0]):
        total = total + pieces[i]
    low = lax.broadcasted_iota(jnp.int32, (TRI, LANES), 1) < BS
    first = total[:TRI]
    second = total[TRI:]
    upper = jnp.where(low, first, pltpu.roll(second, BS, 1)).astype(BF16)
    lower = jnp.where(low, pltpu.roll(first, BS, 1), second).astype(BF16)
    for ref in (out, *(copies.at[g] for g in range(copies.shape[0]))):
        ref[:TRI] = upper
        ref[TRI:] = lower


def merged(pieces):
    return pl.pallas_call(
        merge_kernel,
        in_specs=[pl.BlockSpec(memory_space=pltpu.VMEM)],
        out_specs=[pl.BlockSpec(memory_space=pltpu.VMEM)] * 2,
        out_shape=[
            jax.ShapeDtypeStruct((2 * TRI, LANES), BF16),
            jax.ShapeDtypeStruct((8, 2 * TRI, LANES), BF16),
        ],
        compiler_params=pltpu.CompilerParams(vmem_limit_bytes=16 << 20),
        name="merged",
    )(pieces)


def exchange(pieces, axes, order):
    return lax.all_to_all(
        pieces, axes, 0, 0, axis_index_groups=[list(order)], tiled=True
    )


def local(blocks, ownership, basis_rows):
    core = lax.axis_index("gx_1").astype(jnp.int32).reshape(1)
    kept, sent = local_products(blocks, ownership, basis_rows.T, core)
    arrived = lax.ppermute(sent, "gx_1", [(0, 1), (1, 0)])
    pair = (kept[0] + arrived.astype(F32)).astype(BF16)
    ranks = [4 * y + x for y in ORDER_Y for x in ORDER_X]
    pieces = exchange(pair.reshape(16, 2 * ROWS, LANES), ("gx_0", "gz"), ranks)
    plane = pieces.astype(F32).sum(axis=0)
    plane = plane.reshape(2 * TRI, BLK, LANES).swapaxes(0, 1)
    rounded, copies = merged(exchange(plane, "gy", ORDER_Z))
    gathered = exchange(copies, ("gx_0", "gx_1"), ORDER_YC)
    pieces = exchange(gram_part(rounded, gathered), ("gy", "gz"), ORDER_ZX)
    return pieces.astype(F32).sum(axis=0)


def solution(mesh):
    axes = ("gx_0", "gx_1", "gy", "gz")
    split = Mesh(mesh.devices.reshape(4, 2, mesh.shape["gy"], mesh.shape["gz"]), axes)
    return jax.shard_map(
        local,
        mesh=split,
        in_specs=(P(axes, None, None), P(axes, None), P()),
        out_specs=P(axes, None),
        check_vma=False,
    )
```

```python
import jax
import jax.numpy as jnp
from jax import lax
from jax.experimental import pallas as pl
from jax.experimental.pallas import tpu as pltpu
from jax.sharding import Mesh
from jax.sharding import PartitionSpec as P

NB = 16
R = 48
BS = 64
HALF = BS // 2
QUARTER = BS // 4
PAIRS = R // 2
BLK = 8
QB = R // BLK
TRI = QB * (QB + 1) // 2
ROWS = TRI * BLK
LANES = 2 * BS
STRIDE = 105
CHUNK = 4
F32 = jnp.float32
BF16 = jnp.bfloat16

ORDER_Y = (2, 3, 0, 1)
ORDER_X = (2, 0, 3, 1)
ORDER_Z = (4, 5, 6, 7, 2, 3, 0, 1)
ORDER_YC = (4, 5, 6, 7, 2, 3, 0, 1)
ORDER_ZX = tuple(4 * z + x for z in (4, 5, 6, 7, 0, 1, 2, 3) for x in ORDER_X)

NN = (((1,), (0,)), ((), ()))
NT = (((1,), (1,)), ((), ()))
TN = (((0,), (0,)), ((), ()))


def dot(a, b, dims=NN):
    return lax.dot_general(a, b, dims, preferred_element_type=F32)


def local_kernel(
    own, core, blocks, basis_hbm, acc, send,
    stored, basis, arrived, bases, masked, swapped, wide, wide1, wide0, wide2, with_y, with_x,
):
    slots = blocks.shape[0]

    def low(rows):
        return lax.broadcasted_iota(jnp.int32, (rows, LANES), 1) < BS

    def tile(i):
        return slice(i * LANES, (i + 1) * LANES)

    def paired(first, second):
        mask = low(first.shape[0])
        return (
            jnp.where(mask, first, pltpu.roll(second, BS, 1)),
            jnp.where(mask, pltpu.roll(first, BS, 1), second),
        )

    def row_of_each(ref, row, count=HALF):
        return ref[pl.ds(row, count, stride=STRIDE), :]

    def fetch(slot):
        return pltpu.make_async_copy(blocks.at[slot], stored.at[slot], arrived.at[slot])

    fetch_basis = pltpu.make_async_copy(basis_hbm, basis, arrived.at[slots])
    fetch_basis.start()
    for slot in range(slots):
        fetch(slot).start()
    acc[...] = jnp.zeros_like(acc)
    fetch_basis.wait()
    for j in range(NB // 2):
        columns = basis[:, tile(j)]
        bases[2 * j] = columns[:, :BS]
        bases[2 * j + 1] = columns[:, BS:]

    def each_slot(slot, carry):
        fetch(slot).wait()
        one_slot(slot)
        return carry

    def one_slot(slot):
        v0 = own[0, slot]
        v1 = own[1, slot]
        v2 = own[2, slot]

        @pl.when(v0 >= 0)
        def _():
            u0 = bases[v0]
            u1 = bases[v1]
            u2 = bases[v2]
            zero = jnp.zeros_like(u0)

            def twice(u):
                return jnp.concatenate(
                    [jnp.concatenate([u, zero], 1), jnp.concatenate([zero, u], 1)], 0
                )

            both0 = twice(u0)
            both2 = twice(u2)
            both02 = jnp.concatenate([both0, both2], 1)

            for c in range(HALF // 2):
                first = stored[slot, :, tile(c)].astype(F32)
                second = stored[slot, :, tile(c + HALF // 2)].astype(F32)
                for k, part in enumerate(paired(first, second)):
                    i = 2 * c + k
                    wide[i * STRIDE : i * STRIDE + BS, :] = part
                    masked[:, tile(i)] = part.astype(BF16)

            front = v0 == v1
            back = v1 == v2

            @pl.when(front | back)
            def _():
                x = lax.broadcasted_iota(jnp.int32, (BS, LANES), 0)
                lane = lax.broadcasted_iota(jnp.int32, (BS, LANES), 1)
                z = lane & (BS - 1)
                y_high = jnp.where(lane < BS, 0, HALF)
                order_xy = jnp.where(front, (y_high - x).astype(F32) * 0.5 + 0.5, 2.0 * BS)
                order_yz = jnp.where(back, (z - y_high).astype(F32) * 0.5 + 0.5, 2.0 * BS)

                def scale(i, carry):
                    step = i.astype(F32) * 0.5
                    w = jnp.clip(order_xy + step, 0.0, 1.0) * jnp.clip(order_yz - step, 0.0, 1.0)
                    w = jnp.where(w == 0.25, 1.0 / 6.0, w)
                    rows = pl.ds(i * STRIDE, BS)
                    scaled = wide[rows, :] * w
                    wide[rows, :] = scaled
                    masked[:, pl.ds(pl.multiple_of(i * LANES, LANES), LANES)] = scaled.astype(BF16)
                    return carry

                lax.fori_loop(0, HALF, scale, 0, unroll=4)

            for i in range(HALF):
                upper, lower = paired(row_of_each(wide, i), row_of_each(wide, i + HALF))
                swapped[:HALF, tile(i)] = upper.astype(BF16)
                swapped[HALF:, tile(i)] = lower.astype(BF16)

            def spread(factor, source, ref, target, place):
                for c in range(0, HALF, CHUNK):
                    values = dot(factor, source[:, c * LANES : (c + CHUNK) * LANES])
                    for k in range(CHUNK):
                        start = (c + k) * STRIDE
                        ref[start : start + R, :] = values[:, tile(k)]
                for j in range(PAIRS):
                    upper, lower = paired(row_of_each(ref, 2 * j), row_of_each(ref, 2 * j + 1))
                    target[:HALF, tile(place(j))] = upper.astype(BF16)
                    target[HALF:, tile(place(j))] = lower.astype(BF16)

            spread(u1, swapped, wide1, with_x, lambda j: j)
            spread(u0, masked, wide0, with_y, lambda j: 2 * j + 1)
            for i in range(QUARTER):
                both_tiles = [masked[:, tile(i)], masked[:, tile(i + QUARTER)]]
                wide2[i * STRIDE : i * STRIDE + 2 * R, :] = dot(
                    both2, jnp.concatenate(both_tiles, 0), NT
                )
            for j in range(PAIRS):
                for k in range(2):
                    parts = paired(
                        row_of_each(wide2, k * R + 2 * j, QUARTER),
                        row_of_each(wide2, k * R + 2 * j + 1, QUARTER),
                    )
                    for h in range(2):
                        top = (2 * k + h) * QUARTER
                        with_y[top : top + QUARTER, tile(2 * j)] = parts[h].astype(BF16)

            def place(v):
                group = sum(jnp.where(v // 4 == y, i, 0) for i, y in enumerate(ORDER_Y))
                return ((v // 2) % 2) ^ core[0], group, v % 2

            places = [place(v) for v in (v0, v1, v2)]

            def add(f, j, value):
                side, group, half = places[f]
                block = (side, group, j % 4, half)
                q = j // 4
                start = BLK * (q * (q + 1) // 2)
                rows = BLK * (q + 1)
                at = (*block, slice(start, start + rows), slice(None))
                acc[at] = acc[at] + value[:rows]

            def stacked(ref, tiles):
                return jnp.concatenate([ref[:, t] for t in tiles], 0)

            for q in range(QB):
                g = q // 2
                rows = 2 * BLK * (g + 1)
                tiles = range(4 * q, 4 * q + 4)
                span_y = slice(8 * q * LANES, 8 * (q + 1) * LANES)
                span_x = slice(4 * q * LANES, 4 * (q + 1) * LANES)
                over_y = dot(u1[:rows], with_y[:, span_y])
                over_x = dot(u0[:rows], with_x[:, span_x])
                kept2 = jnp.concatenate([both2[:rows], both2[R : R + rows]], 0)
                kept02 = jnp.concatenate([both02[:rows], both02[R : R + rows]], 0)
                lanes_x = dot(kept2, stacked(with_x, [tile(j) for j in tiles]), NT)
                lanes_y = dot(
                    kept02,
                    stacked(with_y, [slice(2 * j * LANES, (2 * j + 2) * LANES) for j in tiles]),
                    NT,
                )
                for k in range(2):
                    from_x = paired(lanes_x[:rows, tile(k)], lanes_x[rows:, tile(k)])
                    from_y = paired(lanes_y[:rows, tile(k)], lanes_y[rows:, tile(k)])
                    for h in range(2):
                        i = 2 * k + h
                        j = 4 * q + i
                        add(0, j, over_y[:, tile(2 * i)] + from_x[h])
                        add(1, j, from_y[h])
                        add(2, j, over_y[:, tile(2 * i + 1)] + over_x[:, tile(i)])

    lax.fori_loop(0, slots, each_slot, 0)

    def write(m, carry):
        send[m] = acc[1, m].astype(BF16)
        return carry

    lax.fori_loop(0, 4, write, 0)


def in_hbm(array):
    return pltpu.with_memory_space_constraint(array, pltpu.HBM)


def local_products(blocks, ownership, basis, core):
    slots = blocks.shape[0]
    half = (4, 4, 2, ROWS, LANES)
    in_vmem = pl.BlockSpec(memory_space=pltpu.VMEM)
    in_smem = pl.BlockSpec(memory_space=pltpu.SMEM)
    outside = pl.BlockSpec(memory_space=pltpu.HBM)
    return pl.pallas_call(
        local_kernel,
        in_specs=[in_smem, in_smem, outside, outside],
        out_specs=[in_vmem, in_vmem],
        scratch_shapes=[
            pltpu.VMEM(blocks.shape, BF16),
            pltpu.VMEM(basis.shape, BF16),
            pltpu.SemaphoreType.DMA((slots + 1,)),
            pltpu.VMEM((NB, R, BS), BF16),
            pltpu.VMEM((BS, BS * BS), BF16),
            pltpu.VMEM((BS, BS * BS), BF16),
            pltpu.VMEM((HALF * STRIDE, LANES), F32),
            pltpu.VMEM((HALF * STRIDE, LANES), F32),
            pltpu.VMEM((HALF * STRIDE, LANES), F32),
            pltpu.VMEM((QUARTER * STRIDE, LANES), F32),
            pltpu.VMEM((BS, 2 * PAIRS * LANES), BF16),
            pltpu.VMEM((BS, PAIRS * LANES), BF16),
        ],
        out_shape=[
            jax.ShapeDtypeStruct((2, *half), F32),
            jax.ShapeDtypeStruct(half, BF16),
        ],
        compiler_params=pltpu.CompilerParams(vmem_limit_bytes=36 << 20),
        name="local_products",
    )(in_hbm(ownership.T), core, in_hbm(blocks), in_hbm(basis))


def gram_kernel(mine, gathered, out):
    pair = lax.broadcasted_iota(jnp.int32, mine.shape, 0)
    pair = jnp.where(pair < TRI, pair, pair - TRI)
    on_diagonal = pair < 0
    for q in range(QB):
        on_diagonal = on_diagonal | (pair == q * (q + 3) // 2)
    weighted = (mine[...].astype(F32) * jnp.where(on_diagonal, 1.0, 2.0)).astype(BF16)
    everyone = jnp.concatenate([gathered[ORDER_YC.index(g)] for g in range(len(ORDER_YC))], 1)
    gram = dot(weighted, everyone, TN) / R
    for i, place in enumerate(ORDER_ZX):
        out[i] = gram[4 * place : 4 * place + 4].astype(out.dtype)


def gram_part(mine, gathered):
    return pl.pallas_call(
        gram_kernel,
        in_specs=[pl.BlockSpec(memory_space=pltpu.VMEM)] * 2,
        out_specs=pl.BlockSpec(memory_space=pltpu.VMEM),
        out_shape=jax.ShapeDtypeStruct((32, 4, NB * BS), BF16),
        compiler_params=pltpu.CompilerParams(vmem_limit_bytes=16 << 20),
        name="gram_part",
    )(mine, gathered)


def merge_kernel(pieces, out, copies):
    total = pieces[0]
    for i in range(1, pieces.shape[0]):
        total = total + pieces[i]
    low = lax.broadcasted_iota(jnp.int32, (TRI, LANES), 1) < BS
    first = total[:TRI]
    second = total[TRI:]
    upper = jnp.where(low, first, pltpu.roll(second, BS, 1)).astype(BF16)
    lower = jnp.where(low, pltpu.roll(first, BS, 1), second).astype(BF16)
    for ref in (out, *(copies.at[g] for g in range(copies.shape[0]))):
        ref[:TRI] = upper
        ref[TRI:] = lower


def merged(pieces):
    return pl.pallas_call(
        merge_kernel,
        in_specs=[pl.BlockSpec(memory_space=pltpu.VMEM)],
        out_specs=[pl.BlockSpec(memory_space=pltpu.VMEM)] * 2,
        out_shape=[
            jax.ShapeDtypeStruct((2 * TRI, LANES), BF16),
            jax.ShapeDtypeStruct((8, 2 * TRI, LANES), BF16),
        ],
        compiler_params=pltpu.CompilerParams(vmem_limit_bytes=16 << 20),
        name="merged",
    )(pieces)


def exchange(pieces, axes, order):
    return lax.all_to_all(
        pieces, axes, 0, 0, axis_index_groups=[list(order)], tiled=True
    )


def local(blocks, ownership, basis_rows):
    core = lax.axis_index("gx_1").astype(jnp.int32).reshape(1)
    kept, sent = local_products(blocks, ownership, basis_rows.T, core)
    arrived = lax.ppermute(sent, "gx_1", [(0, 1), (1, 0)])
    pair = (kept[0] + arrived.astype(F32)).astype(BF16)
    ranks = [4 * y + x for y in ORDER_Y for x in ORDER_X]
    pieces = exchange(pair.reshape(16, 2 * ROWS, LANES), ("gx_0", "gz"), ranks)
    plane = pieces.astype(F32).sum(axis=0)
    plane = plane.reshape(2 * TRI, BLK, LANES).swapaxes(0, 1)
    rounded, copies = merged(exchange(plane, "gy", ORDER_Z))
    gathered = exchange(copies, ("gx_0", "gx_1"), ORDER_YC)
    pieces = exchange(gram_part(rounded, gathered), ("gy", "gz"), ORDER_ZX)
    return pieces.astype(F32).sum(axis=0)


def solution(mesh):
    axes = ("gx_0", "gx_1", "gy", "gz")
    split = Mesh(mesh.devices.reshape(4, 2, mesh.shape["gy"], mesh.shape["gz"]), axes)
    return jax.shard_map(
        local,
        mesh=split,
        in_specs=(P(axes, None, None), P(axes, None), P()),
        out_specs=P(axes, None),
        check_vma=False,
    )
```

```python
import jax
import jax.numpy as jnp
from jax import lax
from jax.experimental import pallas as pl
from jax.experimental.pallas import tpu as pltpu
from jax.sharding import Mesh
from jax.sharding import PartitionSpec as P

NB = 16
R = 48
BS = 64
HALF = BS // 2
QUARTER = BS // 4
PAIRS = R // 2
BLK = 8
QB = R // BLK
TRI = QB * (QB + 1) // 2
ROWS = TRI * BLK
LANES = 2 * BS
STRIDE = 105
CHUNK = 4
F32 = jnp.float32
BF16 = jnp.bfloat16

ORDER_Y = (2, 3, 0, 1)
ORDER_X = (2, 0, 3, 1)
ORDER_Z = (4, 5, 6, 7, 2, 3, 0, 1)
ORDER_YC = (4, 5, 6, 7, 2, 3, 0, 1)
ORDER_ZX = tuple(4 * z + x for z in (4, 5, 6, 7, 0, 1, 2, 3) for x in ORDER_X)

NN = (((1,), (0,)), ((), ()))
NT = (((1,), (1,)), ((), ()))
TN = (((0,), (0,)), ((), ()))


def dot(a, b, dims=NN):
    return lax.dot_general(a, b, dims, preferred_element_type=F32)


def local_kernel(
    own, core, blocks, basis_hbm, acc, send,
    stored, basis, arrived, bases, masked, swapped, wide, wide1, wide0, wide2, with_y, with_x,
):
    slots = blocks.shape[0]

    def low(rows):
        return lax.broadcasted_iota(jnp.int32, (rows, LANES), 1) < BS

    def tile(i):
        return slice(i * LANES, (i + 1) * LANES)

    def paired(first, second):
        mask = low(first.shape[0])
        return (
            jnp.where(mask, first, pltpu.roll(second, BS, 1)),
            jnp.where(mask, pltpu.roll(first, BS, 1), second),
        )

    def row_of_each(ref, row, count=HALF):
        return ref[pl.ds(row, count, stride=STRIDE), :]

    def fetch(slot):
        return pltpu.make_async_copy(blocks.at[slot], stored.at[slot], arrived.at[slot])

    fetch_basis = pltpu.make_async_copy(basis_hbm, basis, arrived.at[slots])
    fetch_basis.start()
    for slot in range(slots):
        fetch(slot).start()
    acc[...] = jnp.zeros_like(acc)
    fetch_basis.wait()
    for j in range(NB // 2):
        columns = basis[:, tile(j)]
        bases[2 * j] = columns[:, :BS]
        bases[2 * j + 1] = columns[:, BS:]

    def each_slot(slot, carry):
        fetch(slot).wait()
        one_slot(slot)
        return carry

    def one_slot(slot):
        v0 = own[0, slot]
        v1 = own[1, slot]
        v2 = own[2, slot]

        @pl.when(v0 >= 0)
        def _():
            u0 = bases[v0]
            u1 = bases[v1]
            u2 = bases[v2]
            zero = jnp.zeros_like(u0)

            def twice(u):
                return jnp.concatenate(
                    [jnp.concatenate([u, zero], 1), jnp.concatenate([zero, u], 1)], 0
                )

            both0 = twice(u0)
            both2 = twice(u2)
            both02 = jnp.concatenate([both0, both2], 1)

            for c in range(HALF // 2):
                first = stored[slot, :, tile(c)].astype(F32)
                second = stored[slot, :, tile(c + HALF // 2)].astype(F32)
                for k, part in enumerate(paired(first, second)):
                    i = 2 * c + k
                    wide[i * STRIDE : i * STRIDE + BS, :] = part
                    masked[:, tile(i)] = part.astype(BF16)

            front = v0 == v1
            back = v1 == v2

            @pl.when(front | back)
            def _():
                x = lax.broadcasted_iota(jnp.int32, (BS, LANES), 0)
                lane = lax.broadcasted_iota(jnp.int32, (BS, LANES), 1)
                z = lane & (BS - 1)
                y_high = jnp.where(lane < BS, 0, HALF)
                order_xy = jnp.where(front, (y_high - x).astype(F32) * 0.5 + 0.5, 2.0 * BS)
                order_yz = jnp.where(back, (z - y_high).astype(F32) * 0.5 + 0.5, 2.0 * BS)

                def scale(i, carry):
                    step = i.astype(F32) * 0.5
                    w = jnp.clip(order_xy + step, 0.0, 1.0) * jnp.clip(order_yz - step, 0.0, 1.0)
                    w = jnp.where(w == 0.25, 1.0 / 6.0, w)
                    rows = pl.ds(i * STRIDE, BS)
                    scaled = wide[rows, :] * w
                    wide[rows, :] = scaled
                    masked[:, pl.ds(pl.multiple_of(i * LANES, LANES), LANES)] = scaled.astype(BF16)
                    return carry

                lax.fori_loop(0, HALF, scale, 0, unroll=4)

            for i in range(HALF):
                upper, lower = paired(row_of_each(wide, i), row_of_each(wide, i + HALF))
                swapped[:HALF, tile(i)] = upper.astype(BF16)
                swapped[HALF:, tile(i)] = lower.astype(BF16)

            def spread(factor, source, ref, target, place):
                for c in range(0, HALF, CHUNK):
                    values = dot(factor, source[:, c * LANES : (c + CHUNK) * LANES])
                    for k in range(CHUNK):
                        start = (c + k) * STRIDE
                        ref[start : start + R, :] = values[:, tile(k)]
                for j in range(PAIRS):
                    upper, lower = paired(row_of_each(ref, 2 * j), row_of_each(ref, 2 * j + 1))
                    target[:HALF, tile(place(j))] = upper.astype(BF16)
                    target[HALF:, tile(place(j))] = lower.astype(BF16)

            spread(u1, swapped, wide1, with_x, lambda j: j)
            spread(u0, masked, wide0, with_y, lambda j: 2 * j + 1)
            for i in range(QUARTER):
                both_tiles = [masked[:, tile(i)], masked[:, tile(i + QUARTER)]]
                wide2[i * STRIDE : i * STRIDE + 2 * R, :] = dot(
                    both2, jnp.concatenate(both_tiles, 0), NT
                )
            for j in range(PAIRS):
                for k in range(2):
                    parts = paired(
                        row_of_each(wide2, k * R + 2 * j, QUARTER),
                        row_of_each(wide2, k * R + 2 * j + 1, QUARTER),
                    )
                    for h in range(2):
                        top = (2 * k + h) * QUARTER
                        with_y[top : top + QUARTER, tile(2 * j)] = parts[h].astype(BF16)

            def place(v):
                group = sum(jnp.where(v // 4 == y, i, 0) for i, y in enumerate(ORDER_Y))
                return ((v // 2) % 2) ^ core[0], group, v % 2

            places = [place(v) for v in (v0, v1, v2)]

            def add(f, j, value):
                side, group, half = places[f]
                block = (side, group, j % 4, half)
                q = j // 4
                start = BLK * (q * (q + 1) // 2)
                rows = BLK * (q + 1)
                at = (*block, slice(start, start + rows), slice(None))
                acc[at] = acc[at] + value[:rows]

            def stacked(ref, tiles):
                return jnp.concatenate([ref[:, t] for t in tiles], 0)

            for q in range(QB):
                g = q // 2
                rows = 2 * BLK * (g + 1)
                tiles = range(4 * q, 4 * q + 4)
                span_y = slice(8 * q * LANES, 8 * (q + 1) * LANES)
                span_x = slice(4 * q * LANES, 4 * (q + 1) * LANES)
                over_y = dot(u1[:rows], with_y[:, span_y])
                over_x = dot(u0[:rows], with_x[:, span_x])
                kept2 = jnp.concatenate([both2[:rows], both2[R : R + rows]], 0)
                kept02 = jnp.concatenate([both02[:rows], both02[R : R + rows]], 0)
                lanes_x = dot(kept2, stacked(with_x, [tile(j) for j in tiles]), NT)
                lanes_y = dot(
                    kept02,
                    stacked(with_y, [slice(2 * j * LANES, (2 * j + 2) * LANES) for j in tiles]),
                    NT,
                )
                for k in range(2):
                    from_x = paired(lanes_x[:rows, tile(k)], lanes_x[rows:, tile(k)])
                    from_y = paired(lanes_y[:rows, tile(k)], lanes_y[rows:, tile(k)])
                    for h in range(2):
                        i = 2 * k + h
                        j = 4 * q + i
                        add(0, j, over_y[:, tile(2 * i)] + from_x[h])
                        add(1, j, from_y[h])
                        add(2, j, over_y[:, tile(2 * i + 1)] + over_x[:, tile(i)])

    lax.fori_loop(0, slots, each_slot, 0)

    def write(m, carry):
        send[m] = acc[1, m].astype(BF16)
        return carry

    lax.fori_loop(0, 4, write, 0)


def in_hbm(array):
    return pltpu.with_memory_space_constraint(array, pltpu.HBM)


def local_products(blocks, ownership, basis, core):
    slots = blocks.shape[0]
    half = (4, 4, 2, ROWS, LANES)
    in_vmem = pl.BlockSpec(memory_space=pltpu.VMEM)
    in_smem = pl.BlockSpec(memory_space=pltpu.SMEM)
    outside = pl.BlockSpec(memory_space=pltpu.HBM)
    return pl.pallas_call(
        local_kernel,
        in_specs=[in_smem, in_smem, outside, outside],
        out_specs=[in_vmem, in_vmem],
        scratch_shapes=[
            pltpu.VMEM(blocks.shape, BF16),
            pltpu.VMEM(basis.shape, BF16),
            pltpu.SemaphoreType.DMA((slots + 1,)),
            pltpu.VMEM((NB, R, BS), BF16),
            pltpu.VMEM((BS, BS * BS), BF16),
            pltpu.VMEM((BS, BS * BS), BF16),
            pltpu.VMEM((HALF * STRIDE + 112, LANES), F32),
            pltpu.VMEM((HALF * STRIDE + 112, LANES), F32),
            pltpu.VMEM((HALF * STRIDE + 112, LANES), F32),
            pltpu.VMEM((QUARTER * STRIDE + 112, LANES), F32),
            pltpu.VMEM((BS, 2 * PAIRS * LANES), BF16),
            pltpu.VMEM((BS, PAIRS * LANES), BF16),
        ],
        out_shape=[
            jax.ShapeDtypeStruct((2, *half), F32),
            jax.ShapeDtypeStruct(half, BF16),
        ],
        compiler_params=pltpu.CompilerParams(vmem_limit_bytes=36 << 20),
        name="local_products",
    )(in_hbm(ownership.T), core, in_hbm(blocks), in_hbm(basis))


def gram_kernel(mine, gathered, out):
    pair = lax.broadcasted_iota(jnp.int32, mine.shape, 0)
    pair = jnp.where(pair < TRI, pair, pair - TRI)
    on_diagonal = pair < 0
    for q in range(QB):
        on_diagonal = on_diagonal | (pair == q * (q + 3) // 2)
    weighted = (mine[...].astype(F32) * jnp.where(on_diagonal, 1.0, 2.0)).astype(BF16)
    everyone = jnp.concatenate([gathered[ORDER_YC.index(g)] for g in range(len(ORDER_YC))], 1)
    gram = dot(weighted, everyone, TN) / R
    for i, place in enumerate(ORDER_ZX):
        out[i] = gram[4 * place : 4 * place + 4].astype(out.dtype)


def gram_part(mine, gathered):
    return pl.pallas_call(
        gram_kernel,
        in_specs=[pl.BlockSpec(memory_space=pltpu.VMEM)] * 2,
        out_specs=pl.BlockSpec(memory_space=pltpu.VMEM),
        out_shape=jax.ShapeDtypeStruct((32, 4, NB * BS), BF16),
        compiler_params=pltpu.CompilerParams(vmem_limit_bytes=16 << 20),
        name="gram_part",
    )(mine, gathered)


def merge_kernel(pieces, out, copies):
    total = pieces[0]
    for i in range(1, pieces.shape[0]):
        total = total + pieces[i]
    low = lax.broadcasted_iota(jnp.int32, (TRI, LANES), 1) < BS
    first = total[:TRI]
    second = total[TRI:]
    upper = jnp.where(low, first, pltpu.roll(second, BS, 1)).astype(BF16)
    lower = jnp.where(low, pltpu.roll(first, BS, 1), second).astype(BF16)
    for ref in (out, *(copies.at[g] for g in range(copies.shape[0]))):
        ref[:TRI] = upper
        ref[TRI:] = lower


def merged(pieces):
    return pl.pallas_call(
        merge_kernel,
        in_specs=[pl.BlockSpec(memory_space=pltpu.VMEM)],
        out_specs=[pl.BlockSpec(memory_space=pltpu.VMEM)] * 2,
        out_shape=[
            jax.ShapeDtypeStruct((2 * TRI, LANES), BF16),
            jax.ShapeDtypeStruct((8, 2 * TRI, LANES), BF16),
        ],
        compiler_params=pltpu.CompilerParams(vmem_limit_bytes=16 << 20),
        name="merged",
    )(pieces)


def exchange(pieces, axes, order):
    return lax.all_to_all(
        pieces, axes, 0, 0, axis_index_groups=[list(order)], tiled=True
    )


def local(blocks, ownership, basis_rows):
    core = lax.axis_index("gx_1").astype(jnp.int32).reshape(1)
    kept, sent = local_products(blocks, ownership, basis_rows.T, core)
    arrived = lax.ppermute(sent, "gx_1", [(0, 1), (1, 0)])
    pair = (kept[0] + arrived.astype(F32)).astype(BF16)
    ranks = [4 * y + x for y in ORDER_Y for x in ORDER_X]
    pieces = exchange(pair.reshape(16, 2 * ROWS, LANES), ("gx_0", "gz"), ranks)
    plane = pieces.astype(F32).sum(axis=0)
    plane = plane.reshape(2 * TRI, BLK, LANES).swapaxes(0, 1)
    rounded, copies = merged(exchange(plane, "gy", ORDER_Z))
    gathered = exchange(copies, ("gx_0", "gx_1"), ORDER_YC)
    pieces = exchange(gram_part(rounded, gathered), ("gy", "gz"), ORDER_ZX)
    return pieces.astype(F32).sum(axis=0)


def solution(mesh):
    axes = ("gx_0", "gx_1", "gy", "gz")
    split = Mesh(mesh.devices.reshape(4, 2, mesh.shape["gy"], mesh.shape["gz"]), axes)
    return jax.shard_map(
        local,
        mesh=split,
        in_specs=(P(axes, None, None), P(axes, None), P()),
        out_specs=P(axes, None),
        check_vma=False,
    )
```
